32 devices in a mesh: gx: 4 (over y, core), gy: 8 (over z, x).
Axes of the slice: x: 2, y: 2, z: 4, core: 2. Of those that a mesh axis runs over, the one named last changes fastest.
Arguments:
- forcing: float32 [16, 256, 1024], P(None, 'gy', 'gx'), may hold values from -6 to 6
- damping: float32 [16, 256, 1024], P(None, 'gy', 'gx'), may hold values from 0.5 to 4
- coupling: float32 [16, 16], replicated, may hold values from -1.5 to 1.5
- wind_lon: float32 [256, 1024], P('gy', 'gx'), may hold values from -0.5 to 0.5
- wind_lat: float32 [256, 1024], P('gy', 'gx'), may hold values from -0.5 to 0.5
Outputs:
- solution: float32 [16, 256, 1024], P(None, 'gy', 'gx')
- residual: float32 [16, 256, 1024], P(None, 'gy', 'gx')
The draws below stay inside these ranges and needn't reach their ends.
All inputs are finite; a program needn't handle non-finite values.
Results may differ from the reference program's by a relative error of at most 0.0003.
Values sent between devices are 32-bit elements; how exact they have to be, the bound alone decides.
A program may use at most 64 MiB of HBM per device.

```python
import math
import jax
import jax.numpy as jnp
from jax import lax

CH = 16
ITERS = 8
NLAT = 256
NLON = 1024


def block_scale(stream_key, dims, cuts, smallest, high):
    def one(position, parts):
        steps = jax.random.uniform(jax.random.fold_in(jax.random.fold_in(stream_key, 6), position), (parts,), jnp.float32, smallest / len(cuts), high / len(cuts))
        return jnp.repeat(jnp.exp(steps), dims[position] // parts).reshape((-1,) + (1,) * (len(dims) - position - 1))

    factor_of = one(*cuts[0])
    for cut in cuts[1:]:
        factor_of = factor_of * one(*cut)
    return factor_of


def scatter_about(own_key, extent, scale, limit, pieces=(), held_as=jnp.bfloat16):
    factor_of = block_scale(own_key, extent, pieces, -0.22, 0.18) if pieces else 1.0
    drawn = jax.random.normal(own_key, extent, jnp.float32) * scale * factor_of
    return jnp.minimum(jnp.maximum(drawn, -limit), limit).astype(held_as)


def setup_inputs(seed: int = 0) -> dict:
    seeds = jax.random.split(jax.random.key(seed), 6)
    return {
        "forcing": scatter_about(seeds[0], (CH, NLAT, NLON), 1.0, 6.0, ((1, 8), (2, 4)), jnp.float32),
        "damping": jnp.clip(jnp.exp(math.log(4.0) - 2.0794415 * jax.random.uniform(seeds[1], (CH, NLAT, NLON), jnp.float32) ** block_scale(seeds[1], (CH, NLAT, NLON), ((1, 8), (2, 4)), -0.2, 0.2)), 0.5, 4.0),
        "coupling": scatter_about(seeds[2], (CH, CH), CH ** -0.5, 1.5, (), jnp.float32),
        "wind_lon": jnp.clip(jax.random.uniform(seeds[3], (NLAT, NLON), jnp.float32, -0.5, 0.5) * block_scale(seeds[3], (NLAT, NLON), ((0, 8), (1, 4)), -0.4, 0.0), -0.5, 0.5),
        "wind_lat": jnp.clip(jax.random.uniform(seeds[4], (NLAT, NLON), jnp.float32, -0.5, 0.5) * block_scale(seeds[4], (NLAT, NLON), ((0, 8), (1, 4)), -0.4, 0.0), -0.5, 0.5),
    }


COUPLE = 0.25
DIFF_LAT = 0.5
DIFF_LON = 0.5
GUARD = 1.0

def apply_core(padded, damping, coupling, wind_lon, wind_lat, diffuse_lon):
    centre = padded[:, 2:-2, 2:-2]
    east_one = padded[:, 2:-2, 3:-1]
    west_one = padded[:, 2:-2, 1:-3]
    east_two = padded[:, 2:-2, 4:]
    west_two = padded[:, 2:-2, :-4]
    north_one = padded[:, 3:-1, 2:-2]
    south_one = padded[:, 1:-3, 2:-2]
    north_two = padded[:, 4:, 2:-2]
    south_two = padded[:, :-4, 2:-2]
    slope_lon = (8.0 * (east_one - west_one) - (east_two - west_two)) / 12.0
    slope_lat = (8.0 * (north_one - south_one) - (north_two - south_two)) / 12.0
    coupled = COUPLE * jnp.einsum('ij,jab->iab', coupling, centre, precision=lax.Precision.HIGHEST)
    return (1.0 + damping) * centre + coupled + diffuse_lon * (2.0 * centre - east_one - west_one) + DIFF_LAT * (2.0 * centre - north_one - south_one) + wind_lon * slope_lon + wind_lat * slope_lat

def lon_diffusion(row_pos, lat_total):
    phi = -math.pi / 2 + (row_pos + 0.5) * (math.pi / lat_total)
    return DIFF_LON / (jnp.cos(phi) ** 2 + 0.1)

def operate(source, damping, coupling, wind_lon, wind_lat):
    padded = jnp.pad(source, ((0, 0), (2, 2), (0, 0)))
    padded = jnp.concatenate([padded[:, :, -2:], padded, padded[:, :, :2]], axis=2)
    row_pos = jnp.arange(NLAT).astype(jnp.float32)
    diffuse = lon_diffusion(row_pos, NLAT)[:, None]
    return apply_core(padded, damping, coupling, wind_lon, wind_lat, diffuse)

def least_squares(heights, first):
    num_steps = heights.shape[1]
    target = jnp.zeros((num_steps + 1,), jnp.float32).at[0].set(first)
    rotated = heights
    cosines = []
    sines = []
    for column in range(num_steps):
        column_vec = rotated[:, column]
        for earlier in range(column):
            upper_val = column_vec[earlier]
            lower_val = column_vec[earlier + 1]
            column_vec = column_vec.at[earlier].set(cosines[earlier] * upper_val + sines[earlier] * lower_val)
            column_vec = column_vec.at[earlier + 1].set(-sines[earlier] * upper_val + cosines[earlier] * lower_val)
        upper_val = column_vec[column]
        lower_val = column_vec[column + 1]
        radius = jnp.sqrt(upper_val * upper_val + lower_val * lower_val)
        cosine = upper_val / radius
        sine_val = lower_val / radius
        column_vec = column_vec.at[column].set(radius).at[column + 1].set(0.0)
        rotated = rotated.at[:, column].set(column_vec)
        upper_val = target[column]
        lower_val = target[column + 1]
        target = target.at[column].set(cosine * upper_val + sine_val * lower_val)
        target = target.at[column + 1].set(-sine_val * upper_val + cosine * lower_val)
        cosines.append(cosine)
        sines.append(sine_val)
    weights = [None] * num_steps
    for column in reversed(range(num_steps)):
        partial_value = target[column]
        for later_col in range(column + 1, num_steps):
            partial_value = partial_value - rotated[column, later_col] * weights[later_col]
        weights[column] = partial_value / rotated[column, column]
    return weights

def reference(forcing, damping, coupling, wind_lon, wind_lat):
    scale_first = jnp.sqrt(jnp.sum(forcing * forcing) + GUARD)
    krylov = [forcing / scale_first]
    heights = jnp.zeros((ITERS + 1, ITERS), jnp.float32)
    for column in range(ITERS):
        applied = operate(krylov[column], damping, coupling, wind_lon, wind_lat)
        coeffs = jnp.stack([jnp.sum(vector * applied) for vector in krylov])
        for earlier in range(len(krylov)):
            applied = applied - coeffs[earlier] * krylov[earlier]
        subdiag = jnp.sqrt(jnp.sum(applied * applied) + GUARD)
        heights = heights.at[:column + 1, column].set(coeffs).at[column + 1, column].set(subdiag)
        if column + 1 < ITERS:
            krylov.append(applied / subdiag)
    weights = least_squares(heights, scale_first)
    solution = weights[0] * krylov[0]
    for column in range(1, ITERS):
        solution = solution + weights[column] * krylov[column]
    residual = forcing - operate(solution, damping, coupling, wind_lon, wind_lat)
    return (solution, residual)
```

```python
import functools
import math

import jax
import jax.numpy as jnp
from jax import lax
from jax.experimental import pallas as pl
from jax.experimental.pallas import tpu as pltpu
from jax.sharding import PartitionSpec as P

ITERS = 8
COUPLE = 0.25
DIFF_LAT = 0.5
DIFF_LON = 0.5
GUARD = 1.0
MESH = pl.DeviceIdType.MESH
HI = lax.Precision.HIGHEST

MIDDLE = 9.0
RADIUS = 6.0
WIDTH = 3.0
THETA = [MIDDLE + RADIUS * math.cos(math.pi * (2 * k + 1) / (2 * ITERS)) for k in (7, 0, 4, 2, 6, 1, 5, 3)]
PAIRS = [(k, i) for k in range(ITERS + 1) for i in range(k + 1)]
SLOTS = 48


def apply_to(coords):
    out = [None] * (len(coords) + 1)
    for k, value in enumerate(coords):
        low = THETA[k] * value if k < ITERS else value
        out[k] = low if out[k] is None else out[k] + low
        out[k + 1] = WIDTH * value
    return out


def small_solve(gram):
    first = jnp.sqrt(gram[0][0] + GUARD)
    coords = [[1.0 / first]]
    images = [[gram[i][0] * coords[0][0] for i in range(ITERS + 1)]]
    heights = []
    for j in range(ITERS):
        moved = apply_to(coords[j])
        column = []
        for i in range(j + 1):
            column.append(functools.reduce(lambda a, b: a + b, [images[i][k] * moved[k] for k in range(j + 2)]))
        left = list(moved)
        for i in range(j + 1):
            for k in range(i + 1):
                left[k] = left[k] - column[i] * coords[i][k]
        image = [
            functools.reduce(lambda a, b: a + b, [gram[r][k] * left[k] for k in range(j + 2)])
            for r in range(ITERS + 1)
        ]
        norm_sq = functools.reduce(lambda a, b: a + b, [image[k] * left[k] for k in range(j + 2)])
        subdiag = jnp.sqrt(jnp.maximum(norm_sq, 0.0) + GUARD)
        column.append(subdiag)
        heights.append(column)
        inverse = 1.0 / subdiag
        coords.append([v * inverse for v in left])
        images.append([v * inverse for v in image])
    cosines, sines, target, rotated = [], [], [first], []
    for j in range(ITERS):
        column = list(heights[j])
        for e in range(j):
            upper, lower = column[e], column[e + 1]
            column[e] = cosines[e] * upper + sines[e] * lower
            column[e + 1] = cosines[e] * lower - sines[e] * upper
        upper, lower = column[j], column[j + 1]
        radius = jnp.sqrt(upper * upper + lower * lower)
        inverse = 1.0 / radius
        cosine, sine = upper * inverse, lower * inverse
        column[j] = radius
        kept = target[j]
        target[j] = cosine * kept
        target.append(-sine * kept)
        cosines.append(cosine)
        sines.append(sine)
        rotated.append(column)
    weights = [None] * ITERS
    for j in reversed(range(ITERS)):
        value = target[j]
        for later in range(j + 1, ITERS):
            value = value - rotated[later][j] * weights[later]
        weights[j] = value / rotated[j][j]
    answer = [None] * ITERS
    for j in range(ITERS):
        for k in range(j + 1):
            term = weights[j] * coords[j][k]
            answer[k] = term if answer[k] is None else answer[k] + term
    return answer, apply_to(answer)


def kernel(nx, ny, f_hbm, d_hbm, c_ref, wl_ref, wa_ref, kx_ref, sol_hbm, res_hbm,
           basis, diag, coef, block, west_in, east_in, west_out, east_out, gram_acc, mine, slots, splats, outs,
           in_sem, out_sem, lat_send, lat_recv, lon_send, lon_recv, red_send, red_recv):
    channels, lat, lon = f_hbm.shape
    tiles = lon // 128
    total = nx * ny
    ix, iy = lax.axis_index("gx"), lax.axis_index("gy")
    me = ix * ny + iy
    east, west = lax.rem(ix + 1, nx), lax.rem(ix + nx - 1, nx)

    loads = []
    for c in range(channels):
        for q, (src, dst) in enumerate(((f_hbm, basis.at[0]), (d_hbm, diag))):
            off = 2 if q == 0 else 0
            copy = pltpu.make_async_copy(src.at[c], dst.at[pl.ds(off, lat), c, :], in_sem.at[q, c])
            copy.start()
            loads.append(copy)

    barrier = pltpu.get_barrier_semaphore()

    def greet(o, _):
        other = lax.rem(me + o, total)
        pl.semaphore_signal(barrier, inc=1, device_id=(other // ny, lax.rem(other, ny)), device_id_type=MESH)
        return 0

    lax.fori_loop(1, total, greet, 0)

    scale = 1.0 / WIDTH
    row = lax.broadcasted_iota(jnp.int32, (128, channels), 0)
    col = lax.broadcasted_iota(jnp.int32, (128, channels), 1)
    spread = jnp.where(lax.rem(row, channels) == col, 1.0, 0.0).astype(jnp.float32)
    wide = lax.dot_general(spread, c_ref[...], (((1,), (0,)), ((), ())), precision=HI,
                           preferred_element_type=jnp.float32)
    wide = lax.dot_general(wide, spread, (((1,), (1,)), ((), ())), precision=HI,
                           preferred_element_type=jnp.float32)
    same = (lax.broadcasted_iota(jnp.int32, (128, 128), 0) // channels
            == lax.broadcasted_iota(jnp.int32, (128, 128), 1) // channels)
    block[...] = jnp.where(same, wide * (COUPLE * scale), 0.0)
    kx = kx_ref[...] * scale
    wl = wl_ref[...] * (scale / 12.0)
    wa = wa_ref[...] * (scale / 12.0)
    coef[0] = 8.0 * wl - kx
    coef[1] = -8.0 * wl - kx
    coef[2] = wl
    coef[3] = 8.0 * wa - DIFF_LAT * scale
    coef[4] = -8.0 * wa - DIFF_LAT * scale
    coef[5] = wa
    coef[6] = 2.0 * kx + (1.0 + 2.0 * DIFF_LAT) * scale

    def clear(k, _):
        empty = jnp.zeros((2, channels, lon), jnp.float32)

        @pl.when(iy == 0)
        def _():
            basis[k, 0:2] = empty

        @pl.when(iy == ny - 1)
        def _():
            basis[k, lat + 2:lat + 4] = empty

        return 0

    lax.fori_loop(0, ITERS, clear, 0)

    for copy in loads:
        copy.wait()

    def prepare(b, _):
        extra = coef[6, pl.ds(pl.multiple_of(b * 8, 8), 8), :]
        for j in range(8):
            diag[b * 8 + j] = diag[b * 8 + j] * scale + extra[j:j + 1, :]
        return 0

    lax.fori_loop(0, lat // 8, prepare, 0)
    pl.semaphore_wait(barrier, total - 1)

    lane = lax.broadcasted_iota(jnp.int32, (channels, 128), 1)

    def lat_copy(k, way):
        src = pl.ds(lat, 2) if way else pl.ds(2, 2)
        dst = pl.ds(0, 2) if way else pl.ds(lat + 2, 2)
        to = iy + 1 if way else iy - 1
        return pltpu.make_async_remote_copy(
            src_ref=basis.at[k, src], dst_ref=basis.at[k, dst], send_sem=lat_send.at[k, way],
            recv_sem=lat_recv.at[k, way], device_id=(ix, to), device_id_type=MESH)

    def lon_copy(k, way):
        return pltpu.make_async_remote_copy(
            src_ref=(east_out if way else west_out).at[k], dst_ref=(west_in if way else east_in).at[k],
            send_sem=lon_send.at[k, way], recv_sem=lon_recv.at[k, way],
            device_id=(east if way else west, iy), device_id_type=MESH)

    def send(k):
        @pl.when(iy < ny - 1)
        def _():
            lat_copy(k, 1).start()

        @pl.when(iy > 0)
        def _():
            lat_copy(k, 0).start()

        def pack(b, kept):
            to_west, to_east = kept
            for j in range(8):
                r = b * 8 + j
                here = (lane >= 2 * r) & (lane < 2 * r + 2)
                head = basis[k, r + 2, :, 0:128]
                tail = basis[k, r + 2, :, lon - 128:lon]
                to_west = jnp.where(here, pltpu.roll(head, 2 * r, 1), to_west)
                to_east = jnp.where(here, pltpu.roll(tail, lax.rem(2 * r + 2, 128), 1), to_east)
            return to_west, to_east

        empty = jnp.zeros((channels, 128), jnp.float32)
        to_west, to_east = lax.fori_loop(0, lat // 8, pack, (empty, empty))
        west_out[k] = to_west
        east_out[k] = to_east
        lon_copy(k, 0).start()
        lon_copy(k, 1).start()

    def dots(k):
        def one(i, _):
            def part(b, acc):
                acc = list(acc)
                for j in range(8):
                    r = b * 8 + j + 2
                    prod = basis[k, r] * basis[i, r]
                    n = 0
                    for h in range(channels // 8):
                        for t in range(tiles):
                            acc[n % 4] = acc[n % 4] + prod[8 * h:8 * h + 8, 128 * t:128 * t + 128]
                            n += 1
                return tuple(acc)

            zero = jnp.zeros((8, 128), jnp.float32)
            acc = lax.fori_loop(0, lat // 8, part, (zero,) * 4)
            gram_acc[lax.div(k * (k + 1), 2) + i] = (acc[0] + acc[1]) + (acc[2] + acc[3])
            return 0

        lax.fori_loop(0, k + 1, one, 0)

    def rows(k, b, theta):
        from_east, from_west = east_in[k], west_in[k]
        first = b * 8
        stack = jnp.concatenate([basis[k, first + 2 + j] for j in range(8)], axis=0)
        mixed = lax.dot_general(block[...], stack, (((1,), (0,)), ((), ())), precision=HI,
                                preferred_element_type=jnp.float32)
        planes = [coef[q, pl.ds(pl.multiple_of(first, 8), 8), :] for q in range(6)]
        for j in range(8):
            r = first + j
            x = [basis[k, r + 2, :, 128 * t:128 * t + 128] for t in range(tiles)]
            fwd1 = [pltpu.roll(v, 127, 1) for v in x] + [pltpu.roll(from_east, lax.rem(255 - 2 * r, 128), 1)]
            fwd2 = [pltpu.roll(v, 126, 1) for v in x] + [pltpu.roll(from_east, lax.rem(254 - 2 * r, 128), 1)]
            bwd1 = [pltpu.roll(from_west, lax.rem(255 - 2 * r, 128), 1)] + [pltpu.roll(v, 1, 1) for v in x]
            bwd2 = [pltpu.roll(from_west, lax.rem(256 - 2 * r, 128), 1)] + [pltpu.roll(v, 2, 1) for v in x]
            for t in range(tiles):
                cut = slice(128 * t, 128 * t + 128)
                e1 = jnp.where(lane < 127, fwd1[t], fwd1[t + 1])
                e2 = jnp.where(lane < 126, fwd2[t], fwd2[t + 1])
                w1 = jnp.where(lane >= 1, bwd1[t + 1], bwd1[t])
                w2 = jnp.where(lane >= 2, bwd2[t + 1], bwd2[t])

                def weight(q):
                    return planes[q][j:j + 1, cut]

                value = (diag[r, :, cut] - theta) * x[t] + mixed[channels * j:channels * (j + 1), cut]
                value = value + (weight(0) * e1 + weight(1) * w1 + weight(2) * (w2 - e2))
                value = value + (weight(3) * basis[k, r + 3, :, cut] + weight(4) * basis[k, r + 1, :, cut]
                                 + weight(5) * (basis[k, r, :, cut] - basis[k, r + 4, :, cut]))
                basis[k + 1, r + 2, :, cut] = value

    def step(k, _):
        theta = jnp.float32(THETA[0] * scale)
        for i in range(1, ITERS):
            theta = jnp.where(k == i, jnp.float32(THETA[i] * scale), theta)
        send(k)
        dots(k)
        lon_copy(k, 0).wait()
        lon_copy(k, 1).wait()

        def inner(b, _):
            rows(k, b, theta)
            return 0

        lax.fori_loop(1, lat // 8 - 1, inner, 0)

        @pl.when(iy < ny - 1)
        def _():
            lat_copy(k, 1).wait_send()
            lat_copy(k, 0).wait_recv()

        @pl.when(iy > 0)
        def _():
            lat_copy(k, 0).wait_send()
            lat_copy(k, 1).wait_recv()

        def outer(b, _):
            rows(k, b * (lat // 8 - 1), theta)
            return 0

        lax.fori_loop(0, 2, outer, 0)
        return 0

    lax.fori_loop(0, ITERS, step, 0)
    dots(ITERS)

    sums = jnp.concatenate(
        [jnp.sum(gram_acc[n], axis=0, keepdims=True) for n in range(len(PAIRS))]
        + [jnp.zeros((128 - len(PAIRS), 128), jnp.float32)], axis=0)
    flat = lax.dot_general(jnp.ones((8, 128), jnp.float32), sums, (((1,), (1,)), ((), ())), precision=HI,
                           preferred_element_type=jnp.float32)
    mine[...] = flat[0:1, :]
    slots[me] = flat[0:1, :]

    def share(o):
        other = lax.rem(me + o, total)
        return pltpu.make_async_remote_copy(
            src_ref=mine, dst_ref=slots.at[me], send_sem=red_send.at[o], recv_sem=red_recv.at[me],
            device_id=(other // ny, lax.rem(other, ny)), device_id_type=MESH)

    def take(o):
        other = lax.rem(me + total - o, total)
        return pltpu.make_async_remote_copy(
            src_ref=mine, dst_ref=slots.at[other], send_sem=red_send.at[o], recv_sem=red_recv.at[other],
            device_id=(other // ny, lax.rem(other, ny)), device_id_type=MESH)

    def give(o, _):
        share(o).start()
        return 0

    def get(o, _):
        take(o).wait_recv()
        share(o).wait_send()
        return 0

    lax.fori_loop(1, total, give, 0)
    lax.fori_loop(1, total, get, 0)
    whole = slots[0]
    for n in range(1, total):
        whole = whole + slots[n]
    gram = [[None] * (ITERS + 1) for _ in range(ITERS + 1)]
    for n, (k, i) in enumerate(PAIRS):
        gram[k][i] = gram[i][k] = jnp.broadcast_to(whole[:, n:n + 1], (8, 128))
    answer, applied = small_solve(gram)
    for k in range(ITERS):
        splats[k] = answer[k]
    for k in range(ITERS + 1):
        splats[ITERS + k] = applied[k]

    def finish(r, _):
        for h in range(channels // 8):
            for t in range(tiles):
                at = (slice(8 * h, 8 * h + 8), slice(128 * t, 128 * t + 128))
                x = basis[0, r + 2, at[0], at[1]]
                best = splats[0] * x
                rest = x - splats[ITERS] * x
                for k in range(1, ITERS + 1):
                    x = basis[k, r + 2, at[0], at[1]]
                    if k < ITERS:
                        best = best + splats[k] * x
                    rest = rest - splats[ITERS + k] * x
                outs[0, r, at[0], at[1]] = best
                outs[1, r, at[0], at[1]] = rest
        return 0

    lax.fori_loop(0, lat, finish, 0)
    stores = []
    for c in range(channels):
        for q, dst in enumerate((sol_hbm, res_hbm)):
            copy = pltpu.make_async_copy(outs.at[q, :, c, :], dst.at[c], out_sem.at[q, c])
            copy.start()
            stores.append(copy)
    for copy in stores:
        copy.wait()


def solution(mesh):
    nx, ny = mesh.shape["gx"], mesh.shape["gy"]

    def per_device(forcing, damping, coupling, wind_lon, wind_lat):
        channels, lat, lon = forcing.shape
        row_pos = (lax.axis_index("gy") * lat + jnp.arange(lat)).astype(jnp.float32)
        phi = -math.pi / 2 + (row_pos + 0.5) * (math.pi / (lat * ny))
        kx = (DIFF_LON / (jnp.cos(phi) ** 2 + 0.1))[:, None]
        f32 = jnp.float32
        vmem = pl.BlockSpec(memory_space=pltpu.VMEM)
        hbm = pl.BlockSpec(memory_space=pl.ANY)
        dma = pltpu.SemaphoreType.DMA
        shape = jax.ShapeDtypeStruct((channels, lat, lon), f32)
        return pl.pallas_call(
            functools.partial(kernel, nx, ny),
            out_shape=(shape, shape),
            in_specs=[hbm, hbm, vmem, vmem, vmem, vmem],
            out_specs=(hbm, hbm),
            scratch_shapes=[
                pltpu.VMEM((ITERS + 1, lat + 4, channels, lon), f32),
                pltpu.VMEM((lat, channels, lon), f32),
                pltpu.VMEM((7, lat, lon), f32),
                pltpu.VMEM((128, 128), f32),
                pltpu.VMEM((ITERS, channels, 128), f32),
                pltpu.VMEM((ITERS, channels, 128), f32),
                pltpu.VMEM((ITERS, channels, 128), f32),
                pltpu.VMEM((ITERS, channels, 128), f32),
                pltpu.VMEM((len(PAIRS), 8, 128), f32),
                pltpu.VMEM((1, 128), f32),
                pltpu.VMEM((nx * ny, 1, 128), f32),
                pltpu.VMEM((2 * ITERS + 1, 8, 128), f32),
                pltpu.VMEM((2, lat, channels, lon), f32),
                dma((2, channels)), dma((2, channels)),
                dma((ITERS, 2)), dma((ITERS, 2)), dma((ITERS, 2)), dma((ITERS, 2)),
                dma((nx * ny,)), dma((nx * ny,)),
            ],
            compiler_params=pltpu.CompilerParams(
                collective_id=0, has_side_effects=True, vmem_limit_bytes=40 * 1024 * 1024),
        )(forcing, damping, coupling, wind_lon, wind_lat, jnp.broadcast_to(kx, (lat, lon)))

    return jax.shard_map(
        per_device,
        mesh=mesh,
        in_specs=(P(None, "gy", "gx"), P(None, "gy", "gx"), P(), P("gy", "gx"), P("gy", "gx")),
        out_specs=(P(None, "gy", "gx"), P(None, "gy", "gx")),
        check_vma=False,
    )
```

```python
import functools
import math

import jax
import jax.numpy as jnp
from jax import lax
from jax.experimental import pallas as pl
from jax.experimental.pallas import tpu as pltpu
from jax.sharding import PartitionSpec as P

ITERS = 8
COUPLE = 0.25
DIFF_LAT = 0.5
DIFF_LON = 0.5
GUARD = 1.0
MESH = pl.DeviceIdType.MESH
HI = lax.Precision.HIGHEST

MIDDLE = 9.0
RADIUS = 6.0
WIDTH = 3.0
THETA = [MIDDLE + RADIUS * math.cos(math.pi * (2 * k + 1) / (2 * ITERS)) for k in (7, 0, 4, 2, 6, 1, 5, 3)]
PAIRS = [(k, i) for k in range(ITERS + 1) for i in range(k + 1)]
GROUP = 4


def apply_to(coords):
    out = [None] * (len(coords) + 1)
    for k, value in enumerate(coords):
        low = THETA[k] * value if k < ITERS else value
        out[k] = low if out[k] is None else out[k] + low
        out[k + 1] = WIDTH * value
    return out


def small_solve(gram):
    first = jnp.sqrt(gram[0][0] + GUARD)
    coords = [[1.0 / first]]
    images = [[gram[i][0] * coords[0][0] for i in range(ITERS + 1)]]
    heights = []
    for j in range(ITERS):
        moved = apply_to(coords[j])
        column = []
        for i in range(j + 1):
            column.append(functools.reduce(lambda a, b: a + b, [images[i][k] * moved[k] for k in range(j + 2)]))
        left = list(moved)
        for i in range(j + 1):
            for k in range(i + 1):
                left[k] = left[k] - column[i] * coords[i][k]
        image = [
            functools.reduce(lambda a, b: a + b, [gram[r][k] * left[k] for k in range(j + 2)])
            for r in range(ITERS + 1)
        ]
        norm_sq = functools.reduce(lambda a, b: a + b, [image[k] * left[k] for k in range(j + 2)])
        subdiag = jnp.sqrt(jnp.maximum(norm_sq, 0.0) + GUARD)
        column.append(subdiag)
        heights.append(column)
        inverse = 1.0 / subdiag
        coords.append([v * inverse for v in left])
        images.append([v * inverse for v in image])
    cosines, sines, target, rotated = [], [], [first], []
    for j in range(ITERS):
        column = list(heights[j])
        for e in range(j):
            upper, lower = column[e], column[e + 1]
            column[e] = cosines[e] * upper + sines[e] * lower
            column[e + 1] = cosines[e] * lower - sines[e] * upper
        upper, lower = column[j], column[j + 1]
        radius = jnp.sqrt(upper * upper + lower * lower)
        inverse = 1.0 / radius
        cosine, sine = upper * inverse, lower * inverse
        column[j] = radius
        kept = target[j]
        target[j] = cosine * kept
        target.append(-sine * kept)
        cosines.append(cosine)
        sines.append(sine)
        rotated.append(column)
    weights = [None] * ITERS
    for j in reversed(range(ITERS)):
        value = target[j]
        for later in range(j + 1, ITERS):
            value = value - rotated[later][j] * weights[later]
        weights[j] = value / rotated[j][j]
    answer = [None] * ITERS
    for j in range(ITERS):
        for k in range(j + 1):
            term = weights[j] * coords[j][k]
            answer[k] = term if answer[k] is None else answer[k] + term
    return answer, apply_to(answer)


def kernel(nx, ny, f_hbm, d_hbm, c_ref, wl_hbm, wa_hbm, kx_ref, sol_hbm, res_hbm,
           basis, diag, coef, block, west_in, east_in, west_out, east_out, gram_acc, mine, slots, splats, outs, wl_ref, wa_ref,
           in_sem, wind_sem, out_sem, lat_send, lat_recv, lon_send, lon_recv, red_send, red_recv):
    channels, lat, lon = f_hbm.shape
    tiles = lon // 128
    total = nx * ny
    ix, iy = lax.axis_index("gx"), lax.axis_index("gy")
    me = ix * ny + iy
    east, west = lax.rem(ix + 1, nx), lax.rem(ix + nx - 1, nx)

    winds = [pltpu.make_async_copy(wl_hbm, wl_ref, wind_sem.at[0]), pltpu.make_async_copy(wa_hbm, wa_ref, wind_sem.at[1])]
    for copy in winds:
        copy.start()
    loads = []
    for c in range(channels):
        for q, (src, dst) in enumerate(((f_hbm, basis.at[0]), (d_hbm, diag))):
            off = 2 if q == 0 else 0
            copy = pltpu.make_async_copy(src.at[c], dst.at[pl.ds(off, lat), c, :], in_sem.at[q, c])
            copy.start()
            loads.append(copy)

    barrier = pltpu.get_barrier_semaphore()

    def greet(o, _):
        other = lax.rem(me + o, total)
        pl.semaphore_signal(barrier, inc=1, device_id=(other // ny, lax.rem(other, ny)), device_id_type=MESH)
        return 0

    lax.fori_loop(1, total, greet, 0)

    scale = 1.0 / WIDTH
    size = GROUP * channels

    def spread(n):
        row = lax.broadcasted_iota(jnp.int32, (n, channels), 0)
        col = lax.broadcasted_iota(jnp.int32, (n, channels), 1)
        return jnp.where(lax.rem(row, channels) == col, 1.0, 0.0).astype(jnp.float32)

    wide = lax.dot_general(spread(size), c_ref[...], (((1,), (0,)), ((), ())), precision=HI,
                           preferred_element_type=jnp.float32)
    wide = lax.dot_general(wide, spread(3 * size), (((1,), (1,)), ((), ())), precision=HI,
                           preferred_element_type=jnp.float32) * (COUPLE * scale)
    down = lax.broadcasted_iota(jnp.int32, (size, 3 * size), 0)
    across = lax.broadcasted_iota(jnp.int32, (size, 3 * size), 1)
    high = wide.astype(jnp.bfloat16).astype(jnp.float32)
    wide = jnp.where(across < 2 * size, high, wide - high)
    block[...] = jnp.where(down // channels == lax.rem(across, size) // channels, wide, 0.0).astype(jnp.bfloat16)
    for copy in winds:
        copy.wait()
    kx = kx_ref[...] * scale
    wl = wl_ref[...] * (scale / 12.0)
    wa = wa_ref[...] * (scale / 12.0)
    kx = jnp.concatenate([kx] * tiles, axis=1)
    planes = (8.0 * wl - kx, -8.0 * wl - kx, wl, 8.0 * wa - DIFF_LAT * scale, -8.0 * wa - DIFF_LAT * scale, wa,
              2.0 * kx + (1.0 + 2.0 * DIFF_LAT) * scale)
    for q, plane in enumerate(planes):
        for r in range(lat):
            coef[r, q:q + 1, :] = plane[r:r + 1, :]

    for copy in loads:
        copy.wait()

    def prepare(r, _):
        diag[r] = diag[r] * scale + coef[r, 6:7, :]
        return 0

    lax.fori_loop(0, lat, prepare, 0)
    pl.semaphore_wait(barrier, total - 1)

    lane = lax.broadcasted_iota(jnp.int32, (channels, 128), 1)

    def lat_copy(k, way):
        src = pl.ds(lat, 2) if way else pl.ds(2, 2)
        dst = pl.ds(0, 2) if way else pl.ds(lat + 2, 2)
        to = iy + 1 if way else iy - 1
        return pltpu.make_async_remote_copy(
            src_ref=basis.at[k, src], dst_ref=basis.at[k, dst], send_sem=lat_send.at[k, way],
            recv_sem=lat_recv.at[k, way], device_id=(ix, to), device_id_type=MESH)

    def lon_copy(k, way):
        return pltpu.make_async_remote_copy(
            src_ref=(east_out if way else west_out).at[k], dst_ref=(west_in if way else east_in).at[k],
            send_sem=lon_send.at[k, way], recv_sem=lon_recv.at[k, way],
            device_id=(east if way else west, iy), device_id_type=MESH)

    def send_lat(k):
        @pl.when(iy < ny - 1)
        def _():
            lat_copy(k, 1).start()

        @pl.when(iy > 0)
        def _():
            lat_copy(k, 0).start()

    def send_lon(k):
        to_west = to_east = jnp.zeros((channels, 128), jnp.float32)
        for r in range(lat):
            here = (lane >= 2 * r) & (lane < 2 * r + 2)
            head = basis[k, r + 2, :, 0:128]
            tail = basis[k, r + 2, :, lon - 128:lon]
            to_west = jnp.where(here, pltpu.roll(head, 2 * r, 1) if r else head, to_west)
            to_east = jnp.where(here, pltpu.roll(tail, (2 * r + 2) % 128, 1), to_east)
        west_out[k] = to_west
        east_out[k] = to_east
        lon_copy(k, 0).start()
        lon_copy(k, 1).start()

    def dots(k):
        def one(i, _):
            def part(b, acc):
                acc = list(acc)
                for j in range(8):
                    r = b * 8 + j + 2
                    prod = basis[k, r] * basis[i, r]
                    n = 0
                    for h in range(channels // 8):
                        for t in range(tiles):
                            acc[n % 4] = acc[n % 4] + prod[8 * h:8 * h + 8, 128 * t:128 * t + 128]
                            n += 1
                return tuple(acc)

            zero = jnp.zeros((8, 128), jnp.float32)
            acc = lax.fori_loop(0, lat // 8, part, (zero,) * 4)
            gram_acc[lax.div(k * (k + 1), 2) + i] = (acc[0] + acc[1]) + (acc[2] + acc[3])
            return 0

        lax.fori_loop(0, k + 1, one, 0)

    def rows(k, picked, theta):
        from_east, from_west = east_in[k], west_in[k]
        stack = jnp.concatenate([basis[k, r + 2] for r in picked], axis=0)
        high = stack.astype(jnp.bfloat16)
        low = (stack - high.astype(jnp.float32)).astype(jnp.bfloat16)
        mixed = lax.dot_general(block[...], jnp.concatenate([high, low, high], axis=0), (((1,), (0,)), ((), ())),
                                preferred_element_type=jnp.float32)
        for j, r in enumerate(picked):
            x = [basis[k, r + 2, :, 128 * t:128 * t + 128] for t in range(tiles)]
            fwd1 = [pltpu.roll(v, 127, 1) for v in x] + [pltpu.roll(from_east, (255 - 2 * r) % 128, 1)]
            fwd2 = [pltpu.roll(v, 126, 1) for v in x] + [pltpu.roll(from_east, (254 - 2 * r) % 128, 1)]
            bwd1 = [pltpu.roll(from_west, (255 - 2 * r) % 128, 1)] + [pltpu.roll(v, 1, 1) for v in x]
            bwd2 = [pltpu.roll(from_west, (256 - 2 * r) % 128, 1) if r % 64 else from_west] + [pltpu.roll(v, 2, 1) for v in x]
            for t in range(tiles):
                cut = slice(128 * t, 128 * t + 128)
                e1 = jnp.where(lane < 127, fwd1[t], fwd1[t + 1])
                e2 = jnp.where(lane < 126, fwd2[t], fwd2[t + 1])
                w1 = jnp.where(lane >= 1, bwd1[t + 1], bwd1[t])
                w2 = jnp.where(lane >= 2, bwd2[t + 1], bwd2[t])

                def weight(q):
                    return coef[r, q:q + 1, cut]

                value = (diag[r, :, cut] - theta) * x[t] + mixed[channels * j:channels * (j + 1), cut]
                value = value + (weight(0) * e1 + weight(1) * w1 + weight(2) * (w2 - e2))
                if r + 1 < lat:
                    value = value + weight(3) * basis[k, r + 3, :, cut]
                if r >= 1:
                    value = value + weight(4) * basis[k, r + 1, :, cut]
                south = basis[k, r, :, cut] if r >= 2 else None
                north = basis[k, r + 4, :, cut] if r + 2 < lat else None
                if south is None:
                    value = value - weight(5) * north
                elif north is None:
                    value = value + weight(5) * south
                else:
                    value = value + weight(5) * (south - north)
                basis[k + 1, r + 2, :, cut] = value

    def step(k, _):
        theta = jnp.float32(THETA[0] * scale)
        for i in range(1, ITERS):
            theta = jnp.where(k == i, jnp.float32(THETA[i] * scale), theta)
        dots(k)
        lon_copy(k, 0).wait()
        lon_copy(k, 1).wait()

        rows(k, (0, 1, lat - 2, lat - 1), theta)

        @pl.when(iy > 0)
        def _():
            lat_copy(k, 1).wait_recv()
            basis[k + 1, 2] += coef[0, 4:5, :] * basis[k, 1] + coef[0, 5:6, :] * basis[k, 0]
            basis[k + 1, 3] += coef[1, 5:6, :] * basis[k, 1]

            @pl.when(k + 1 < ITERS)
            def _():
                lat_copy(k + 1, 0).start()

            lat_copy(k, 0).wait_send()

        @pl.when(iy < ny - 1)
        def _():
            lat_copy(k, 0).wait_recv()
            near = basis[k, lat + 2]
            basis[k + 1, lat + 1] += coef[lat - 1, 3:4, :] * near - coef[lat - 1, 5:6, :] * basis[k, lat + 3]
            basis[k + 1, lat] -= coef[lat - 2, 5:6, :] * near

            @pl.when(k + 1 < ITERS)
            def _():
                lat_copy(k + 1, 1).start()

            lat_copy(k, 1).wait_send()

        for b in range((lat - 4) // GROUP):
            rows(k, [2 + GROUP * b + j for j in range(GROUP)], theta)

        @pl.when(k + 1 < ITERS)
        def _():
            send_lon(k + 1)

        return 0

    send_lat(0)
    send_lon(0)
    lax.fori_loop(0, ITERS, step, 0)
    dots(ITERS)

    sums = jnp.concatenate(
        [jnp.sum(gram_acc[n], axis=0, keepdims=True) for n in range(len(PAIRS))]
        + [jnp.zeros((128 - len(PAIRS), 128), jnp.float32)], axis=0)
    flat = lax.dot_general(jnp.ones((8, 128), jnp.float32), sums, (((1,), (1,)), ((), ())), precision=HI,
                           preferred_element_type=jnp.float32)
    mine[...] = flat[0:1, :]
    slots[me] = flat[0:1, :]

    def share(o):
        other = lax.rem(me + o, total)
        return pltpu.make_async_remote_copy(
            src_ref=mine, dst_ref=slots.at[me], send_sem=red_send.at[o], recv_sem=red_recv.at[me],
            device_id=(other // ny, lax.rem(other, ny)), device_id_type=MESH)

    def take(o):
        other = lax.rem(me + total - o, total)
        return pltpu.make_async_remote_copy(
            src_ref=mine, dst_ref=slots.at[other], send_sem=red_send.at[o], recv_sem=red_recv.at[other],
            device_id=(other // ny, lax.rem(other, ny)), device_id_type=MESH)

    def give(o, _):
        share(o).start()
        return 0

    def get(o, _):
        take(o).wait_recv()
        share(o).wait_send()
        return 0

    lax.fori_loop(1, total, give, 0)
    lax.fori_loop(1, total, get, 0)
    whole = slots[0]
    for n in range(1, total):
        whole = whole + slots[n]
    gram = [[None] * (ITERS + 1) for _ in range(ITERS + 1)]
    for n, (k, i) in enumerate(PAIRS):
        gram[k][i] = gram[i][k] = jnp.broadcast_to(whole[:, n:n + 1], (8, 128))
    answer, applied = small_solve(gram)
    for k in range(ITERS):
        splats[k] = answer[k]
    for k in range(ITERS + 1):
        splats[ITERS + k] = applied[k]

    def finish(r, _):
        for h in range(channels // 8):
            for t in range(tiles):
                at = (slice(8 * h, 8 * h + 8), slice(128 * t, 128 * t + 128))
                x = basis[0, r + 2, at[0], at[1]]
                best = splats[0] * x
                rest = x - splats[ITERS] * x
                for k in range(1, ITERS + 1):
                    x = basis[k, r + 2, at[0], at[1]]
                    if k < ITERS:
                        best = best + splats[k] * x
                    rest = rest - splats[ITERS + k] * x
                outs[0, r, at[0], at[1]] = best
                outs[1, r, at[0], at[1]] = rest
        return 0

    lax.fori_loop(0, lat, finish, 0)
    stores = []
    for c in range(channels):
        for q, dst in enumerate((sol_hbm, res_hbm)):
            copy = pltpu.make_async_copy(outs.at[q, :, c, :], dst.at[c], out_sem.at[q, c])
            copy.start()
            stores.append(copy)
    for copy in stores:
        copy.wait()


def solution(mesh):
    nx, ny = mesh.shape["gx"], mesh.shape["gy"]

    def per_device(forcing, damping, coupling, wind_lon, wind_lat):
        channels, lat, lon = forcing.shape
        row_pos = (lax.axis_index("gy") * lat + jnp.arange(lat)).astype(jnp.float32)
        phi = -math.pi / 2 + (row_pos + 0.5) * (math.pi / (lat * ny))
        kx = (DIFF_LON / (jnp.cos(phi) ** 2 + 0.1))[:, None]
        f32 = jnp.float32
        vmem = pl.BlockSpec(memory_space=pltpu.VMEM)
        hbm = pl.BlockSpec(memory_space=pl.ANY)
        dma = pltpu.SemaphoreType.DMA
        shape = jax.ShapeDtypeStruct((channels, lat, lon), f32)
        return pl.pallas_call(
            functools.partial(kernel, nx, ny),
            out_shape=(shape, shape),
            in_specs=[hbm, hbm, vmem, hbm, hbm, vmem],
            out_specs=(hbm, hbm),
            scratch_shapes=[
                pltpu.VMEM((ITERS + 1, lat + 4, channels, lon), f32),
                pltpu.VMEM((lat, channels, lon), f32),
                pltpu.VMEM((lat, 8, lon), f32),
                pltpu.VMEM((GROUP * channels, 3 * GROUP * channels), jnp.bfloat16),
                pltpu.VMEM((ITERS, channels, 128), f32),
                pltpu.VMEM((ITERS, channels, 128), f32),
                pltpu.VMEM((ITERS, channels, 128), f32),
                pltpu.VMEM((ITERS, channels, 128), f32),
                pltpu.VMEM((len(PAIRS), 8, 128), f32),
                pltpu.VMEM((1, 128), f32),
                pltpu.VMEM((nx * ny, 1, 128), f32),
                pltpu.VMEM((2 * ITERS + 1, 8, 128), f32),
                pltpu.VMEM((2, lat, channels, lon), f32),
                pltpu.VMEM((lat, lon), f32), pltpu.VMEM((lat, lon), f32),
                dma((2, channels)), dma((2,)), dma((2, channels)),
                dma((ITERS, 2)), dma((ITERS, 2)), dma((ITERS, 2)), dma((ITERS, 2)),
                dma((nx * ny,)), dma((nx * ny,)),
            ],
            compiler_params=pltpu.CompilerParams(
                collective_id=0, has_side_effects=True, vmem_limit_bytes=63 * 1024 * 1024),
        )(forcing, damping, coupling, wind_lon, wind_lat, jnp.broadcast_to(kx, (lat, 128)))

    return jax.shard_map(
        per_device,
        mesh=mesh,
        in_specs=(P(None, "gy", "gx"), P(None, "gy", "gx"), P(), P("gy", "gx"), P("gy", "gx")),
        out_specs=(P(None, "gy", "gx"), P(None, "gy", "gx")),
        check_vma=False,
    )
```

```python
import functools
import math

import jax
import jax.numpy as jnp
from jax import lax
from jax.experimental import pallas as pl
from jax.experimental.pallas import tpu as pltpu
from jax.sharding import PartitionSpec as P

ITERS = 8
COUPLE = 0.25
DIFF_LAT = 0.5
DIFF_LON = 0.5
GUARD = 1.0
MESH = pl.DeviceIdType.MESH
HI = lax.Precision.HIGHEST

MIDDLE = 9.0
RADIUS = 6.0
WIDTH = 3.0
THETA = [MIDDLE + RADIUS * math.cos(math.pi * (2 * k + 1) / (2 * ITERS)) for k in (7, 0, 4, 2, 6, 1, 5, 3)]
PAIRS = [(k, i) for k in range(ITERS + 1) for i in range(k + 1)]
GROUP = 4


def apply_to(coords):
    out = [None] * (len(coords) + 1)
    for k, value in enumerate(coords):
        low = THETA[k] * value if k < ITERS else value
        out[k] = low if out[k] is None else out[k] + low
        out[k + 1] = WIDTH * value
    return out


def small_solve(gram):
    first = jnp.sqrt(gram[0][0] + GUARD)
    coords = [[1.0 / first]]
    images = [[gram[i][0] * coords[0][0] for i in range(ITERS + 1)]]
    heights = []
    for j in range(ITERS):
        moved = apply_to(coords[j])
        column = []
        for i in range(j + 1):
            column.append(functools.reduce(lambda a, b: a + b, [images[i][k] * moved[k] for k in range(j + 2)]))
        left = list(moved)
        for i in range(j + 1):
            for k in range(i + 1):
                left[k] = left[k] - column[i] * coords[i][k]
        image = [
            functools.reduce(lambda a, b: a + b, [gram[r][k] * left[k] for k in range(j + 2)])
            for r in range(ITERS + 1)
        ]
        norm_sq = functools.reduce(lambda a, b: a + b, [image[k] * left[k] for k in range(j + 2)])
        subdiag = jnp.sqrt(jnp.maximum(norm_sq, 0.0) + GUARD)
        column.append(subdiag)
        heights.append(column)
        inverse = 1.0 / subdiag
        coords.append([v * inverse for v in left])
        images.append([v * inverse for v in image])
    cosines, sines, target, rotated = [], [], [first], []
    for j in range(ITERS):
        column = list(heights[j])
        for e in range(j):
            upper, lower = column[e], column[e + 1]
            column[e] = cosines[e] * upper + sines[e] * lower
            column[e + 1] = cosines[e] * lower - sines[e] * upper
        upper, lower = column[j], column[j + 1]
        radius = jnp.sqrt(upper * upper + lower * lower)
        inverse = 1.0 / radius
        cosine, sine = upper * inverse, lower * inverse
        column[j] = radius
        kept = target[j]
        target[j] = cosine * kept
        target.append(-sine * kept)
        cosines.append(cosine)
        sines.append(sine)
        rotated.append(column)
    weights = [None] * ITERS
    for j in reversed(range(ITERS)):
        value = target[j]
        for later in range(j + 1, ITERS):
            value = value - rotated[later][j] * weights[later]
        weights[j] = value / rotated[j][j]
    answer = [None] * ITERS
    for j in range(ITERS):
        for k in range(j + 1):
            term = weights[j] * coords[j][k]
            answer[k] = term if answer[k] is None else answer[k] + term
    return answer, apply_to(answer)


def kernel(nx, ny, f_hbm, d_hbm, c_ref, wl_hbm, wa_hbm, kx_ref, sol_hbm, res_hbm,
           basis, diag, coef, block, west_in, east_in, west_out, east_out, gram_acc, mine, slots, splats, outs, wl_ref, wa_ref,
           in_sem, wind_sem, out_sem, lat_send, lat_recv, lon_send, lon_recv, red_send, red_recv):
    channels, lat, lon = f_hbm.shape
    tiles = lon // 128
    total = nx * ny
    ix, iy = lax.axis_index("gx"), lax.axis_index("gy")
    me = ix * ny + iy
    east, west = lax.rem(ix + 1, nx), lax.rem(ix + nx - 1, nx)

    winds = [pltpu.make_async_copy(wl_hbm, wl_ref, wind_sem.at[0]), pltpu.make_async_copy(wa_hbm, wa_ref, wind_sem.at[1])]
    for copy in winds:
        copy.start()
    loads = []
    for c in range(channels):
        for q, (src, dst) in enumerate(((f_hbm, basis.at[0]), (d_hbm, diag))):
            off = 2 if q == 0 else 0
            copy = pltpu.make_async_copy(src.at[c], dst.at[pl.ds(off, lat), c, :], in_sem.at[q, c])
            copy.start()
            loads.append(copy)

    barrier = pltpu.get_barrier_semaphore()

    def greet(o, _):
        other = lax.rem(me + o, total)
        pl.semaphore_signal(barrier, inc=1, device_id=(other // ny, lax.rem(other, ny)), device_id_type=MESH)
        return 0

    lax.fori_loop(1, total, greet, 0)

    scale = 1.0 / WIDTH
    size = GROUP * channels

    def spread(n):
        row = lax.broadcasted_iota(jnp.int32, (n, channels), 0)
        col = lax.broadcasted_iota(jnp.int32, (n, channels), 1)
        return jnp.where(lax.rem(row, channels) == col, 1.0, 0.0).astype(jnp.float32)

    wide = lax.dot_general(spread(size), c_ref[...], (((1,), (0,)), ((), ())), precision=HI,
                           preferred_element_type=jnp.float32)
    wide = lax.dot_general(wide, spread(3 * size), (((1,), (1,)), ((), ())), precision=HI,
                           preferred_element_type=jnp.float32) * (COUPLE * scale)
    down = lax.broadcasted_iota(jnp.int32, (size, 3 * size), 0)
    across = lax.broadcasted_iota(jnp.int32, (size, 3 * size), 1)
    high = wide.astype(jnp.bfloat16).astype(jnp.float32)
    wide = jnp.where(across < 2 * size, high, wide - high)
    block[...] = jnp.where(down // channels == lax.rem(across, size) // channels, wide, 0.0).astype(jnp.bfloat16)
    for copy in winds:
        copy.wait()
    kx = kx_ref[...] * scale
    wl = wl_ref[...] * (scale / 12.0)
    wa = wa_ref[...] * (scale / 12.0)
    kx = jnp.concatenate([kx] * tiles, axis=1)
    planes = (8.0 * wl - kx, -8.0 * wl - kx, wl, 8.0 * wa - DIFF_LAT * scale, -8.0 * wa - DIFF_LAT * scale, wa,
              2.0 * kx + (1.0 + 2.0 * DIFF_LAT) * scale)
    for q, plane in enumerate(planes):
        for r in range(lat):
            coef[r, q:q + 1, :] = plane[r:r + 1, :]

    for copy in loads[0::2]:
        copy.wait()

    pl.semaphore_wait(barrier, total - 1)

    lane = lax.broadcasted_iota(jnp.int32, (channels, 128), 1)

    def lat_copy(k, way):
        src = pl.ds(lat, 2) if way else pl.ds(2, 2)
        dst = pl.ds(0, 2) if way else pl.ds(lat + 2, 2)
        to = iy + 1 if way else iy - 1
        return pltpu.make_async_remote_copy(
            src_ref=basis.at[k, src], dst_ref=basis.at[k, dst], send_sem=lat_send.at[k, way],
            recv_sem=lat_recv.at[k, way], device_id=(ix, to), device_id_type=MESH)

    def lon_copy(k, way):
        return pltpu.make_async_remote_copy(
            src_ref=(east_out if way else west_out).at[k], dst_ref=(west_in if way else east_in).at[k],
            send_sem=lon_send.at[k, way], recv_sem=lon_recv.at[k, way],
            device_id=(east if way else west, iy), device_id_type=MESH)

    def send_lat(k):
        @pl.when(iy < ny - 1)
        def _():
            lat_copy(k, 1).start()

        @pl.when(iy > 0)
        def _():
            lat_copy(k, 0).start()

    def send_lon(k):
        to_west = to_east = jnp.zeros((channels, 128), jnp.float32)
        for r in range(lat):
            here = (lane >= 2 * r) & (lane < 2 * r + 2)
            head = basis[k, r + 2, :, 0:128]
            tail = basis[k, r + 2, :, lon - 128:lon]
            to_west = jnp.where(here, pltpu.roll(head, 2 * r, 1) if r else head, to_west)
            to_east = jnp.where(here, pltpu.roll(tail, (2 * r + 2) % 128, 1), to_east)
        west_out[k] = to_west
        east_out[k] = to_east
        lon_copy(k, 0).start()
        lon_copy(k, 1).start()

    def dots(k):
        def one(i, _):
            def part(b, acc):
                acc = list(acc)
                for j in range(8):
                    r = b * 8 + j + 2
                    prod = basis[k, r] * basis[i, r]
                    n = 0
                    for h in range(channels // 8):
                        for t in range(tiles):
                            acc[n % 4] = acc[n % 4] + prod[8 * h:8 * h + 8, 128 * t:128 * t + 128]
                            n += 1
                return tuple(acc)

            zero = jnp.zeros((8, 128), jnp.float32)
            acc = lax.fori_loop(0, lat // 8, part, (zero,) * 4)
            gram_acc[lax.div(k * (k + 1), 2) + i] = (acc[0] + acc[1]) + (acc[2] + acc[3])
            return 0

        lax.fori_loop(0, k + 1, one, 0)

    def rows(k, picked, theta):
        from_east, from_west = east_in[k], west_in[k]
        stack = jnp.concatenate([basis[k, r + 2] for r in picked], axis=0)
        high = stack.astype(jnp.bfloat16)
        low = (stack - high.astype(jnp.float32)).astype(jnp.bfloat16)
        mixed = lax.dot_general(block[...], jnp.concatenate([high, low, high], axis=0), (((1,), (0,)), ((), ())),
                                preferred_element_type=jnp.float32)
        for j, r in enumerate(picked):
            x = [basis[k, r + 2, :, 128 * t:128 * t + 128] for t in range(tiles)]
            fwd1 = [pltpu.roll(v, 127, 1) for v in x] + [pltpu.roll(from_east, (255 - 2 * r) % 128, 1)]
            fwd2 = [pltpu.roll(v, 126, 1) for v in x] + [pltpu.roll(from_east, (254 - 2 * r) % 128, 1)]
            bwd1 = [pltpu.roll(from_west, (255 - 2 * r) % 128, 1)] + [pltpu.roll(v, 1, 1) for v in x]
            bwd2 = [pltpu.roll(from_west, (256 - 2 * r) % 128, 1) if r % 64 else from_west] + [pltpu.roll(v, 2, 1) for v in x]
            for t in range(tiles):
                cut = slice(128 * t, 128 * t + 128)
                e1 = jnp.where(lane < 127, fwd1[t], fwd1[t + 1])
                e2 = jnp.where(lane < 126, fwd2[t], fwd2[t + 1])
                w1 = jnp.where(lane >= 1, bwd1[t + 1], bwd1[t])
                w2 = jnp.where(lane >= 2, bwd2[t + 1], bwd2[t])

                def weight(q):
                    return coef[r, q:q + 1, cut]

                value = (diag[r, :, cut] - theta) * x[t] + mixed[channels * j:channels * (j + 1), cut]
                value = value + (weight(0) * e1 + weight(1) * w1 + weight(2) * (w2 - e2))
                if r + 1 < lat:
                    value = value + weight(3) * basis[k, r + 3, :, cut]
                if r >= 1:
                    value = value + weight(4) * basis[k, r + 1, :, cut]
                south = basis[k, r, :, cut] if r >= 2 else None
                north = basis[k, r + 4, :, cut] if r + 2 < lat else None
                if south is None:
                    value = value - weight(5) * north
                elif north is None:
                    value = value + weight(5) * south
                else:
                    value = value + weight(5) * (south - north)
                basis[k + 1, r + 2, :, cut] = value

    def step(k, _):
        theta = jnp.float32(THETA[0] * scale)
        for i in range(1, ITERS):
            theta = jnp.where(k == i, jnp.float32(THETA[i] * scale), theta)
        dots(k)
        lon_copy(k, 0).wait()
        lon_copy(k, 1).wait()

        rows(k, (0, 1, lat - 2, lat - 1), theta)

        @pl.when(iy > 0)
        def _():
            lat_copy(k, 1).wait_recv()
            basis[k + 1, 2] += coef[0, 4:5, :] * basis[k, 1] + coef[0, 5:6, :] * basis[k, 0]
            basis[k + 1, 3] += coef[1, 5:6, :] * basis[k, 1]

            @pl.when(k + 1 < ITERS)
            def _():
                lat_copy(k + 1, 0).start()

            lat_copy(k, 0).wait_send()

        @pl.when(iy < ny - 1)
        def _():
            lat_copy(k, 0).wait_recv()
            near = basis[k, lat + 2]
            basis[k + 1, lat + 1] += coef[lat - 1, 3:4, :] * near - coef[lat - 1, 5:6, :] * basis[k, lat + 3]
            basis[k + 1, lat] -= coef[lat - 2, 5:6, :] * near

            @pl.when(k + 1 < ITERS)
            def _():
                lat_copy(k + 1, 1).start()

            lat_copy(k, 1).wait_send()

        for b in range((lat - 4) // GROUP):
            rows(k, [2 + GROUP * b + j for j in range(GROUP)], theta)

        @pl.when(k + 1 < ITERS)
        def _():
            send_lon(k + 1)

        return 0

    send_lat(0)
    send_lon(0)
    for copy in loads[1::2]:
        copy.wait()

    def prepare(r, _):
        diag[r] = diag[r] * scale + coef[r, 6:7, :]
        return 0

    lax.fori_loop(0, lat, prepare, 0)
    lax.fori_loop(0, ITERS, step, 0)
    dots(ITERS)

    sums = jnp.concatenate(
        [jnp.sum(gram_acc[n], axis=0, keepdims=True) for n in range(len(PAIRS))]
        + [jnp.zeros((128 - len(PAIRS), 128), jnp.float32)], axis=0)
    flat = lax.dot_general(jnp.ones((8, 128), jnp.float32), sums, (((1,), (1,)), ((), ())), precision=HI,
                           preferred_element_type=jnp.float32)
    mine[...] = flat[0:1, :]
    slots[me] = flat[0:1, :]

    def share(o):
        other = lax.rem(me + o, total)
        return pltpu.make_async_remote_copy(
            src_ref=mine, dst_ref=slots.at[me], send_sem=red_send.at[o], recv_sem=red_recv.at[me],
            device_id=(other // ny, lax.rem(other, ny)), device_id_type=MESH)

    def take(o):
        other = lax.rem(me + total - o, total)
        return pltpu.make_async_remote_copy(
            src_ref=mine, dst_ref=slots.at[other], send_sem=red_send.at[o], recv_sem=red_recv.at[other],
            device_id=(other // ny, lax.rem(other, ny)), device_id_type=MESH)

    def give(o, _):
        share(o).start()
        return 0

    def get(o, _):
        take(o).wait_recv()
        share(o).wait_send()
        return 0

    lax.fori_loop(1, total, give, 0)
    lax.fori_loop(1, total, get, 0)
    whole = slots[0]
    for n in range(1, total):
        whole = whole + slots[n]
    gram = [[None] * (ITERS + 1) for _ in range(ITERS + 1)]
    for n, (k, i) in enumerate(PAIRS):
        gram[k][i] = gram[i][k] = jnp.broadcast_to(whole[:, n:n + 1], (8, 128))
    answer, applied = small_solve(gram)
    for k in range(ITERS):
        splats[k] = answer[k]
    for k in range(ITERS + 1):
        splats[ITERS + k] = applied[k]

    def store(q, c, b):
        some = pl.ds(pl.multiple_of(b * 8, 8), 8)
        return pltpu.make_async_copy(outs.at[q, some, c, :], (sol_hbm, res_hbm)[q].at[c, some, :], out_sem.at[q, c, b])

    def finish(b, _):
        for j in range(8):
            r = b * 8 + j
            for h in range(channels // 8):
                for t in range(tiles):
                    at = (slice(8 * h, 8 * h + 8), slice(128 * t, 128 * t + 128))
                    x = basis[0, r + 2, at[0], at[1]]
                    best = splats[0] * x
                    rest = x - splats[ITERS] * x
                    for k in range(1, ITERS + 1):
                        x = basis[k, r + 2, at[0], at[1]]
                        if k < ITERS:
                            best = best + splats[k] * x
                        rest = rest - splats[ITERS + k] * x
                    outs[0, r, at[0], at[1]] = best
                    outs[1, r, at[0], at[1]] = rest
        for q in range(2):
            for c in range(channels):
                store(q, c, b).start()
        return 0

    def drain(b, _):
        for q in range(2):
            for c in range(channels):
                store(q, c, b).wait()
        return 0

    lax.fori_loop(0, lat // 8, finish, 0)
    lax.fori_loop(0, lat // 8, drain, 0)


def solution(mesh):
    nx, ny = mesh.shape["gx"], mesh.shape["gy"]

    def per_device(forcing, damping, coupling, wind_lon, wind_lat):
        channels, lat, lon = forcing.shape
        row_pos = (lax.axis_index("gy") * lat + jnp.arange(lat)).astype(jnp.float32)
        phi = -math.pi / 2 + (row_pos + 0.5) * (math.pi / (lat * ny))
        kx = (DIFF_LON / (jnp.cos(phi) ** 2 + 0.1))[:, None]
        f32 = jnp.float32
        vmem = pl.BlockSpec(memory_space=pltpu.VMEM)
        hbm = pl.BlockSpec(memory_space=pl.ANY)
        dma = pltpu.SemaphoreType.DMA
        shape = jax.ShapeDtypeStruct((channels, lat, lon), f32)
        return pl.pallas_call(
            functools.partial(kernel, nx, ny),
            out_shape=(shape, shape),
            in_specs=[hbm, hbm, vmem, hbm, hbm, vmem],
            out_specs=(hbm, hbm),
            scratch_shapes=[
                pltpu.VMEM((ITERS + 1, lat + 4, channels, lon), f32),
                pltpu.VMEM((lat, channels, lon), f32),
                pltpu.VMEM((lat, 8, lon), f32),
                pltpu.VMEM((GROUP * channels, 3 * GROUP * channels), jnp.bfloat16),
                pltpu.VMEM((ITERS, channels, 128), f32),
                pltpu.VMEM((ITERS, channels, 128), f32),
                pltpu.VMEM((ITERS, channels, 128), f32),
                pltpu.VMEM((ITERS, channels, 128), f32),
                pltpu.VMEM((len(PAIRS), 8, 128), f32),
                pltpu.VMEM((1, 128), f32),
                pltpu.VMEM((nx * ny, 1, 128), f32),
                pltpu.VMEM((2 * ITERS + 1, 8, 128), f32),
                pltpu.VMEM((2, lat, channels, lon), f32),
                pltpu.VMEM((lat, lon), f32), pltpu.VMEM((lat, lon), f32),
                dma((2, channels)), dma((2,)), dma((2, channels, lat // 8)),
                dma((ITERS, 2)), dma((ITERS, 2)), dma((ITERS, 2)), dma((ITERS, 2)),
                dma((nx * ny,)), dma((nx * ny,)),
            ],
            compiler_params=pltpu.CompilerParams(
                collective_id=0, has_side_effects=True, vmem_limit_bytes=63 * 1024 * 1024),
        )(forcing, damping, coupling, wind_lon, wind_lat, jnp.broadcast_to(kx, (lat, 128)))

    return jax.shard_map(
        per_device,
        mesh=mesh,
        in_specs=(P(None, "gy", "gx"), P(None, "gy", "gx"), P(), P("gy", "gx"), P("gy", "gx")),
        out_specs=(P(None, "gy", "gx"), P(None, "gy", "gx")),
        check_vma=False,
    )
```
